256 devices in a mesh: dp: 32 (over y, z), group: 8 (over x, core).
Axes of the slice: x: 4, y: 4, z: 8, core: 2. Of those that a mesh axis runs over, the one named last changes fastest.
Arguments:
- rewards: bfloat16 [65536, 4096], P(('dp', 'group')), may hold values from -6 to 6
- values: bfloat16 [65536, 4096], P(('dp', 'group')), may hold values from -6 to 6
- lengths: int32 [65536], P(('dp', 'group')), may hold values from 1 to 4096
- decay_rate: float32 [65536], P(('dp', 'group')), may hold values from 3.8146973e-06 to 0.03125
- piece_dest: int32 [32, 32], P('dp'), may hold values from 0 to 31, each once within a row
- row_perm: int32 [512, 128], P(('dp', 'group')), may hold values from 0 to 127, each once within a row
- minibatch: int32 [65536], P(('dp', 'group')), may hold values from 0 to 63
Outputs:
- white_rewards: bfloat16 [65536, 4096], P(('dp', 'group'))
- white_advantage: bfloat16 [65536, 4096], P(('dp', 'group'))
The draws below stay inside these ranges and needn't reach their ends.
Inputs may be any that keep to these rules, and one draw needn't show every extreme that they name: Each row of piece_dest names every index of dp once. Each row of row_perm names every number below 128 once.
All inputs are finite; a program needn't handle non-finite values.
Results may differ from the reference program's by a relative error of at most 0.0049.
Values may be sent and summed in bfloat16 or wider, within the bound.
No kernel may reach another device: no remote copies, remote signals or barrier semaphores. Data moves between devices by JAX's collectives and lax.ppermute only.
A program may use at most 64 MiB of HBM per device.

```python
import math
import jax
import jax.numpy as jnp
from jax import lax

LEN = 4096
BLK = 128
ROWS_DEV = 256
MINIBATCHES = 64
ROWS = 65536
BLOCKS = 512
N_DP = 32
N_GROUP = 8


def plant(result, rng, least, high):
    shape = result.shape
    index_at = [jax.random.randint(jax.random.fold_in(rng, axis), (), 0, shape[axis]) for axis in range(len(shape))]
    result = result.at[tuple(index_at)].set(least)
    longest = shape.index(max(shape))
    index_at[longest] = (index_at[longest] + 1) % shape[longest]
    return result.at[tuple(index_at)].set(high)


def shard_levels(rng, dims, pieces, least, high):
    gain, own = 1.0, jax.random.fold_in(rng, 6)
    for dim, blocks in pieces:
        heights = jnp.exp(jax.random.uniform(jax.random.fold_in(own, dim), (blocks,), jnp.float32, least / len(pieces), high / len(pieces)))
        gain = gain * jnp.repeat(heights, dims[dim] // blocks).reshape([-1 if axis == dim else 1 for axis in range(len(dims))])
    return gain


def centred(key, extent, scale, most, pieces=(), kind=jnp.bfloat16):
    entries = scale * jax.random.normal(key, extent, jnp.float32)
    if pieces:
        entries = entries * shard_levels(key, extent, pieces, -0.22, 0.18)
    return jnp.clip(entries, -most, most).astype(kind)


def setup_inputs(seed: int = 0) -> dict:
    streams_of = jax.random.split(jax.random.key(seed), 8)
    return {
        "rewards": centred(streams_of[0], (ROWS, LEN), 1.0, 6.0, ((0, 256),)),
        "values": centred(streams_of[1], (ROWS, LEN), 1.0, 6.0, ((0, 256),)),
        "lengths": plant(jax.random.randint(streams_of[2], (ROWS,), 1, LEN + 1), jax.random.fold_in(streams_of[2], 1), 1, LEN).astype(jnp.int32),
        "decay_rate": jnp.clip(jnp.exp(math.log(0.03125) - 9.010913 * jax.random.uniform(streams_of[3], (ROWS,), jnp.float32) ** shard_levels(streams_of[3], (ROWS,), ((0, 256),), -0.2, 0.2)), 3.814697265625e-06, 0.03125),
        "piece_dest": jax.vmap(lambda own: jax.random.permutation(own, N_DP))(jax.random.split(streams_of[4], N_DP)).reshape((N_DP, N_DP)).astype(jnp.int32),
        "row_perm": jax.vmap(lambda own: jax.random.permutation(own, BLK))(jax.random.split(streams_of[5], BLOCKS)).reshape((BLOCKS, BLK)).astype(jnp.int32),
        "minibatch": plant(jax.random.randint(streams_of[6], (ROWS,), 0, MINIBATCHES), jax.random.fold_in(streams_of[6], 1), 0, MINIBATCHES - 1).astype(jnp.int32),
    }


def reference(rewards, values, lengths, decay_rate, piece_dest, row_perm, minibatch):
    rows_all, span_all = rewards.shape
    position = jnp.arange(span_all, dtype=jnp.int32)
    is_valid = position[None, :] < lengths[:, None]
    next_valid = position[None, :] + 1 < lengths[:, None]
    per_step = jnp.exp(-decay_rate)
    value_f = values.astype(jnp.float32)
    value_next = jnp.concatenate([value_f[:, 1:], jnp.zeros((rows_all, 1), jnp.float32)], axis=1)
    td_error = rewards.astype(jnp.float32) + per_step[:, None] * jnp.where(next_valid, value_next, 0.0) - value_f
    td_error = jnp.where(is_valid, td_error, 0.0)

    def backward(carry, column):
        fresh = column + per_step * carry
        return (fresh, fresh)
    starting = jnp.zeros((rows_all,), jnp.float32)
    final_carry, stacked = lax.scan(backward, starting, td_error.T, reverse=True)
    advantage = stacked.T.astype(jnp.bfloat16)
    piece = ROWS_DEV // N_DP
    source_slot = jnp.argsort(piece_dest, axis=1).astype(jnp.int32)
    out_rows = jnp.arange(rows_all, dtype=jnp.int32)
    device = out_rows // ROWS_DEV
    target = device // N_GROUP
    column_group = device % N_GROUP
    inside = out_rows % ROWS_DEV
    chosen = inside // BLK * BLK + row_perm.reshape(-1).astype(jnp.int32)
    source_dev = chosen // piece
    within = chosen % piece
    source_row = (source_dev * N_GROUP + column_group) * ROWS_DEV + source_slot[source_dev, target] * piece + within
    moved_rewards = jnp.take(rewards, source_row, axis=0).astype(jnp.float32)
    moved_advantage = jnp.take(advantage, source_row, axis=0).astype(jnp.float32)
    moved_lengths = jnp.take(lengths, source_row, axis=0)
    valid = position[None, :] < moved_lengths[:, None]
    moved_rewards = jnp.where(valid, moved_rewards, 0.0)
    moved_advantage = jnp.where(valid, moved_advantage, 0.0)
    count = jax.ops.segment_sum(moved_lengths.astype(jnp.float32), minibatch, num_segments=MINIBATCHES)
    count = jnp.maximum(count, 1.0)

    def whiten(moved):
        mean = jax.ops.segment_sum(lax.optimization_barrier(jnp.sum(moved, axis=1)), minibatch, num_segments=MINIBATCHES) / count
        deviation = jnp.where(valid, moved - mean[minibatch][:, None], 0.0)
        spread = jax.ops.segment_sum(lax.optimization_barrier(jnp.sum(deviation * deviation, axis=1)), minibatch, num_segments=MINIBATCHES) / count
        return (deviation / jnp.sqrt(spread[minibatch][:, None] + 1e-05)).astype(jnp.bfloat16)
    return (whiten(moved_rewards), whiten(moved_advantage))
```

```python
import functools

import jax
import jax.numpy as jnp
from jax import lax
from jax.experimental import pallas as pl
from jax.experimental.pallas import tpu as pltpu
from jax.sharding import Mesh
from jax.sharding import PartitionSpec as P

MINIBATCHES = 64
NY, NZ = 4, 8
PIECE = 8
DP_GROUP = ("dp_0", "dp_1", "group_0", "group_1")
DP = ("dp_0", "dp_1")
HIGHEST = lax.Precision.HIGHEST
Z_ORDER = (1, 7, 2, 6, 3, 5, 4)
Y_ORDER = (1, 3, 2)
ANY = pl.ANY


def shift(dy, dz):
    return [
        (y * NZ + z, ((y + dy) % NY) * NZ + (z + dz) % NZ) for y in range(NY) for z in range(NZ)
    ]


def staged(pairs, held, arrived, left):
    inward = [
        pltpu.make_async_copy(source, held.at[n], arrived.at[n])
        for n, (source, _) in enumerate(pairs)
    ]
    outward = [
        pltpu.make_async_copy(held.at[n], target, left.at[n])
        for n, (_, target) in enumerate(pairs)
    ]
    for copy in inward:
        copy.start()
    for first, second in zip(inward, outward):
        first.wait()
        second.start()
    for copy in outward:
        copy.wait()


def copy_pieces_body(table, source, *rest):
    outs, (held, arrived, left) = rest[:-3], rest[-3:]
    targets = [out.at[slot] for out in outs for slot in range(out.shape[0])]
    staged([(source.at[table[n]], target) for n, target in enumerate(targets)], held, arrived, left)


def staging(count, piece, dtype):
    return [
        pltpu.VMEM((count,) + piece, dtype),
        pltpu.SemaphoreType.DMA((count,)),
        pltpu.SemaphoreType.DMA((count,)),
    ]


def copy_pieces(table, source, counts):
    piece = source.shape[1:]
    return pl.pallas_call(
        copy_pieces_body,
        out_shape=[jax.ShapeDtypeStruct((n,) + piece, source.dtype) for n in counts],
        in_specs=[pl.BlockSpec(memory_space=pltpu.SMEM), pl.BlockSpec(memory_space=ANY)],
        out_specs=[pl.BlockSpec(memory_space=ANY) for _ in counts],
        scratch_shapes=staging(sum(counts), piece, source.dtype),
        name="copy_pieces",
    )(table, source)


def rebucket(parts):
    before, after = len(parts), parts[0].shape[0]
    piece = parts[0].shape[1:]

    def body(*refs):
        ins, outs = refs[:before], refs[before : before + after]
        pairs = [(ins[j].at[k], outs[k].at[j]) for k in range(after) for j in range(before)]
        staged(pairs, *refs[before + after :])

    return pl.pallas_call(
        body,
        out_shape=[jax.ShapeDtypeStruct((before,) + piece, parts[0].dtype) for _ in range(after)],
        in_specs=[pl.BlockSpec(memory_space=ANY) for _ in parts],
        out_specs=[pl.BlockSpec(memory_space=ANY) for _ in range(after)],
        scratch_shapes=staging(before * after, piece, parts[0].dtype),
        name="rebucket",
    )(*parts)


LANE = 128
CHUNK = 512


def advantage_body(
    table, rewards, values, lengths, rate, out0, out1, out2, out3, stats, carry, low, up, reach, acc
):
    step = pl.program_id(0)
    steps = pl.num_programs(0)
    chunk = steps - 1 - step
    outs = (out0, out1, out2, out3)
    rows = lengths.shape[0]
    lane = lax.broadcasted_iota(jnp.int32, (rows, LANE), 1)

    @pl.when(step == 0)
    def _():
        offset = lane.astype(jnp.float32)
        wide = jnp.broadcast_to(rate[...], (rows, LANE))
        low[...] = jnp.exp(-wide * offset)
        up[...] = jnp.exp(wide * offset)
        reach[...] = jnp.exp(-wide * (LANE - offset))
        carry[...] = jnp.zeros_like(carry)
        acc[...] = jnp.zeros_like(acc)

    triangle = (
        lax.broadcasted_iota(jnp.int32, (LANE, LANE), 0)
        >= lax.broadcasted_iota(jnp.int32, (LANE, LANE), 1)
    ).astype(jnp.float32).astype(jnp.bfloat16)
    left = lengths[...] - chunk * CHUNK
    head = carry[...]
    pieces = table.shape[0]
    sources = [table[s] for s in range(pieces)]

    def gathered(ref, cols):
        return jnp.concatenate([ref[s, :, cols].astype(jnp.float32) for s in sources], axis=0)

    for block in reversed(range(CHUNK // LANE)):
        cols = slice(block * LANE, (block + 1) * LANE)
        valid = lane < left - block * LANE
        reward = jnp.where(valid, gathered(rewards, cols), 0.0)
        scaled = reward * low[...]
        high = scaled.astype(jnp.bfloat16)
        rest = (scaled - high.astype(jnp.float32)).astype(jnp.bfloat16)
        summed = jnp.dot(high, triangle, preferred_element_type=jnp.float32) + jnp.dot(
            rest, triangle, preferred_element_type=jnp.float32
        )
        total = summed * up[...] + reach[...] * head
        head = jnp.broadcast_to(total[:, 0:1], (rows, LANE))
        kept = jnp.where(valid, total - gathered(values, cols), 0.0).astype(jnp.bfloat16)
        kept_f = kept.astype(jnp.float32)
        acc[0] += reward
        acc[1] += kept_f
        acc[2] += reward * reward
        acc[3] += kept_f * kept_f
        for s in range(pieces):
            outs[s // NZ][s % NZ, :, cols] = kept_f[s * PIECE : (s + 1) * PIECE].astype(jnp.bfloat16)
    carry[...] = head

    @pl.when(step == steps - 1)
    def _():
        result = jnp.where(lane == 0, lengths[...].astype(jnp.float32), 0.0)
        for term in range(4):
            result = jnp.where(
                lane == term + 1, jnp.sum(acc[term], axis=1, keepdims=True), result
            )
        stats[...] = result


def advantage_sends(table, rewards, values, lengths, rate):
    pieces, piece, span = rewards.shape
    rows = pieces * piece
    steps = span // CHUNK

    def at_chunk(i):
        return (0, 0, steps - 1 - i)

    def fixed(i):
        return (0, 0)

    return pl.pallas_call(
        advantage_body,
        grid=(steps,),
        out_shape=[jax.ShapeDtypeStruct((NZ, piece, span), jnp.bfloat16) for _ in range(NY)]
        + [jax.ShapeDtypeStruct((rows, LANE), jnp.float32)],
        in_specs=[
            pl.BlockSpec(memory_space=pltpu.SMEM),
            pl.BlockSpec((pieces, piece, CHUNK), at_chunk),
            pl.BlockSpec((pieces, piece, CHUNK), at_chunk),
            pl.BlockSpec((rows, 1), fixed),
            pl.BlockSpec((rows, 1), fixed),
        ],
        out_specs=[pl.BlockSpec((NZ, piece, CHUNK), at_chunk) for _ in range(NY)]
        + [pl.BlockSpec((rows, LANE), fixed)],
        scratch_shapes=[pltpu.VMEM((rows, LANE), jnp.float32) for _ in range(4)]
        + [pltpu.VMEM((4, rows, LANE), jnp.float32)],
        compiler_params=pltpu.CompilerParams(dimension_semantics=("arbitrary",)),
        name="advantage_sends",
    )(table, rewards, values, lengths, rate)


WIDE = 1024


def whiten_body(column, lengths, mean, scale, *refs):
    parts, out = refs[:-1], refs[-1]
    chunk = pl.program_id(0)
    rows = lengths.shape[0]
    chooser = (
        lax.broadcasted_iota(jnp.int32, (rows, rows), 1) == column[...]
    ).astype(jnp.float32).astype(jnp.bfloat16)
    held = jnp.concatenate([part[...] for part in parts], axis=0)
    mixed = jnp.dot(chooser, held, preferred_element_type=jnp.float32)
    position = chunk * WIDE + lax.broadcasted_iota(jnp.int32, (rows, WIDE), 1)
    white = jnp.where(position < lengths[...], (mixed - mean[...]) * scale[...], 0.0)
    out[...] = white.astype(jnp.bfloat16)


def whitened(column, lengths, mean, scale, parts):
    rows, span = lengths.shape[0], parts[0].shape[1]

    def fixed(i):
        return (0, 0)

    def at_chunk(i):
        return (0, i)

    return pl.pallas_call(
        whiten_body,
        grid=(span // WIDE,),
        out_shape=jax.ShapeDtypeStruct((rows, span), jnp.bfloat16),
        in_specs=[pl.BlockSpec((rows, 1), fixed) for _ in range(4)]
        + [pl.BlockSpec((part.shape[0], WIDE), at_chunk) for part in parts],
        out_specs=pl.BlockSpec((rows, WIDE), at_chunk),
        compiler_params=pltpu.CompilerParams(dimension_semantics=("arbitrary",)),
        name="whitened",
    )(column, lengths, mean, scale, *parts)


def local(rewards, values, lengths, decay_rate, piece_dest, row_perm, minibatch):
    rows, span = rewards.shape
    blocks_here, block = row_perm.shape
    peers = piece_dest.shape[1]
    here_y = lax.axis_index("dp_0")
    here_z = lax.axis_index("dp_1")
    slots = jnp.arange(peers, dtype=jnp.int32)
    target = piece_dest[0]
    source_slot = jnp.sum(jnp.where(target[None, :] == slots[:, None], slots[None, :], 0), axis=1)
    shifted = ((slots // NZ + here_y) % NY) * NZ + (slots + here_z) % NZ
    ring_slot = jnp.sum(jnp.where(target[None, :] == shifted[:, None], slots[None, :], 0), axis=1)
    ring_pick = target[None, :] == shifted[:, None]
    piece_lengths = lengths.reshape(peers, PIECE)
    piece_rates = decay_rate.reshape(peers, PIECE)
    ring_lengths = jnp.sum(jnp.where(ring_pick[:, :, None], piece_lengths[None], 0), axis=1)
    ring_rates = jnp.sum(jnp.where(ring_pick[:, :, None], piece_rates[None], 0.0), axis=1)
    sent_lengths = jnp.sum(
        jnp.where((target[None, :] == slots[:, None])[:, :, None], piece_lengths[None], 0), axis=1
    )
    within = jnp.arange(block, dtype=jnp.int32)
    picks = row_perm[:, :, None] == within[None, None, :]
    ids_received = jnp.sum(
        jnp.where(picks, minibatch.reshape(blocks_here, block)[:, :, None], 0), axis=1
    )
    small = jnp.concatenate([sent_lengths, ids_received.reshape(peers, PIECE)], axis=1)
    small = lax.all_to_all(
        small.astype(jnp.float32), DP, split_axis=0, concat_axis=0, tiled=True
    ).astype(jnp.int32)
    lengths_received = small[:, :PIECE].reshape(blocks_here, 1, block)
    lengths_here = jnp.sum(jnp.where(picks, lengths_received, 0), axis=2).reshape(rows, 1)

    pieces = rewards.reshape(peers, PIECE, span)
    (reward_sends,) = copy_pieces(source_slot, pieces, (peers,))
    moved_rewards = lax.all_to_all(reward_sends, DP, split_axis=0, concat_axis=0, tiled=True)

    *advantage_parts, row_terms = advantage_sends(
        ring_slot,
        pieces,
        values.reshape(peers, PIECE, span),
        ring_lengths.reshape(rows, 1),
        ring_rates.reshape(rows, 1),
    )
    across_y = list(advantage_parts)
    for j in Y_ORDER:
        across_y[j] = lax.ppermute(advantage_parts[j], DP, shift(j, 0))
    bundles = rebucket(across_y)
    across_z = list(bundles)
    for k in Z_ORDER:
        across_z[k] = lax.ppermute(bundles[k], DP, shift(0, k))

    ids_sent = small[:, PIECE:].reshape(NY, NZ, PIECE)
    ids_sent = lax.dynamic_slice_in_dim(jnp.concatenate([ids_sent, ids_sent], 0), here_y, NY, 0)
    ids_sent = lax.dynamic_slice_in_dim(jnp.concatenate([ids_sent, ids_sent], 1), here_z, NZ, 1)
    groups = jnp.arange(MINIBATCHES, dtype=jnp.int32)
    member_sent = (ids_sent.reshape(rows)[None, :] == groups[:, None]).astype(jnp.float32)
    totals = jnp.dot(member_sent, row_terms[:, :8], precision=HIGHEST)
    totals = lax.psum(totals, "group_1")
    totals = lax.psum(totals, "group_0")
    totals = totals + sum(lax.ppermute(totals, DP, shift(j, 0)) for j in Y_ORDER)
    totals = totals + sum(lax.ppermute(totals, DP, shift(0, k)) for k in Z_ORDER)
    count = jnp.maximum(totals[:, 0], 1.0)
    means = totals[:, 1:3] / count[:, None]
    spreads = jnp.maximum(totals[:, 3:5] / count[:, None] - means * means, 0.0)
    per_group = jnp.concatenate([means, lax.rsqrt(spreads + 1e-05)], axis=1)
    member = (minibatch[:, None] == groups[None, :]).astype(jnp.float32)
    per_row = jnp.dot(member, per_group, precision=HIGHEST)

    new_order = (jnp.arange(blocks_here, dtype=jnp.int32)[:, None] * block + row_perm).reshape(-1)
    from_dev = new_order // PIECE
    from_j = (here_y - from_dev // NZ) % NY
    from_k = (here_z - from_dev % NZ) % NZ
    ring_column = (from_k * NY + from_j) * PIECE + new_order % PIECE
    white_rewards = whitened(
        new_order[:, None],
        lengths_here,
        per_row[:, 0:1],
        per_row[:, 2:3],
        [moved_rewards.reshape(rows, span)],
    )
    white_advantage = whitened(
        ring_column[:, None],
        lengths_here,
        per_row[:, 1:2],
        per_row[:, 3:4],
        [part.reshape(NY * PIECE, span) for part in across_z],
    )
    return (white_rewards, white_advantage)


def solution(mesh):
    finer = Mesh(mesh.devices.reshape(4, 8, 4, 2), DP_GROUP)
    placed = (
        P(DP_GROUP, None),
        P(DP_GROUP, None),
        P(DP_GROUP),
        P(DP_GROUP),
        P(DP, None),
        P(DP_GROUP, None),
        P(DP_GROUP),
    )
    return jax.shard_map(
        local,
        mesh=finer,
        in_specs=placed,
        out_specs=(P(DP_GROUP, None), P(DP_GROUP, None)),
        check_vma=False,
    )
```
